256 devices in a mesh: resp: 8 (over y, x_lo), ctx: 32 (over x_hi, z, core).
Axes of the slice: x: 4 (x_hi: 2, x_lo: 2; x = x_hi * 2 + x_lo), y: 4, z: 8, core: 2. Of those that a mesh axis runs over, the one named last changes fastest.
Arguments:
- prompt_queries: bfloat16 [32, 512, 640], P('ctx', 'resp'), may hold values from -10 to 10
- prompt_keys: bfloat16 [32, 512, 128], P('ctx', 'resp'), may hold values from -6 to 6
- prompt_values: bfloat16 [32, 512, 128], P('ctx', 'resp'), may hold values from -18 to 18
- response_queries: bfloat16 [16, 1536, 640], P('resp', 'ctx'), may hold values from -10 to 10
- response_keys: bfloat16 [16, 1536, 128], P('resp', 'ctx'), may hold values from -6 to 6
- response_values: bfloat16 [16, 1536, 128], P('resp', 'ctx'), may hold values from -18 to 18
- response_lengths: int32 [16], P('resp'), may hold values from 384 to 1536, as said below
Outputs:
- prompt_output: bfloat16 [32, 512, 640], P('ctx', 'resp')
- response_output: bfloat16 [16, 1536, 640], P('resp', 'ctx')
The draws below stay inside these ranges and needn't reach their ends.
Inputs may be any that keep to these rules, and one draw needn't show every extreme that they name: `response_lengths`: some response has all 1536 positions live.
All inputs are finite; a program needn't handle non-finite values.
Results may differ from the reference program's by a relative error of at most 0.006.
Values may be sent and summed in bfloat16 or wider, within the bound.
No kernel may reach another device: no remote copies, remote signals or barrier semaphores. Data moves between devices by JAX's collectives and lax.ppermute only.
A program may use at most 64 MiB of HBM per device.

```python
import jax
import jax.numpy as jnp
from jax import lax

DH = 128
HQ = 5
P_DEV = 512
L_DEV = 48
L = 1536
RESPONSES = 16
N_CTX = 32


def draw_prompt_keys(key, part):
    row_count = N_CTX * P_DEV
    own_key = jax.random.fold_in(key, 11)
    key_rows = jnp.clip(jax.random.normal(own_key, (row_count, DH), jnp.float32), -6.0, 6.0)
    return key_rows.reshape(N_CTX, P_DEV, DH).astype(jnp.bfloat16)


def draw_prompt_queries(key, part):
    row_count = N_CTX * P_DEV
    own_key = jax.random.fold_in(key, 21)
    query_rows = jnp.clip(2.5 * jax.random.normal(own_key, (row_count, HQ * DH), jnp.float32), -10.0, 10.0)
    return query_rows.reshape(N_CTX, P_DEV, HQ * DH).astype(jnp.bfloat16)


def draw_response_queries(key, part):
    row_count = RESPONSES * N_CTX * L_DEV
    own_key = jax.random.fold_in(key, 41)
    query_rows = jnp.clip(2.5 * jax.random.normal(own_key, (row_count, HQ * DH), jnp.float32), -10.0, 10.0)
    return query_rows.reshape(RESPONSES, N_CTX * L_DEV, HQ * DH).astype(jnp.bfloat16)


def draw_response_lengths(key, part):
    whole_length = N_CTX * L_DEV
    lengths = jax.random.randint(jax.random.fold_in(key, 31), (RESPONSES,), whole_length // 4, whole_length + 1)
    longest = jax.random.randint(jax.random.fold_in(key, 32), (), 0, RESPONSES)
    return lengths.at[longest].set(whole_length).astype(jnp.int32)


def shard_levels(key, extent, shards, least, top_value):
    def one(position, blocks):
        steps = jax.random.uniform(jax.random.fold_in(jax.random.fold_in(key, 6), position), (blocks,), jnp.float32, least / len(shards), top_value / len(shards))
        return jnp.repeat(jnp.exp(steps), extent[position] // blocks).reshape((-1,) + (1,) * (len(extent) - position - 1))

    level = one(*shards[0])
    for cut in shards[1:]:
        level = level * one(*cut)
    return level


def noise(stream_key, extent, width, limit, shards=(), kind=jnp.bfloat16):
    values = jax.random.normal(stream_key, extent, jnp.float32) * width
    if len(shards) > 0:
        values = shard_levels(stream_key, extent, shards, -0.22, 0.18) * values
    return jnp.clip(values, min=-limit, max=limit).astype(kind)


def setup_inputs(seed: int = 0) -> dict:
    seeds = jax.random.split(jax.random.key(seed), 8)
    prompt_queries = draw_prompt_queries(jax.random.fold_in(seeds[7], 71), 0)
    prompt_keys = draw_prompt_keys(jax.random.fold_in(seeds[7], 71), 0)
    prompt_values = noise(seeds[2], (N_CTX, P_DEV, DH), 3.0, 18.0, ((0, 32), (1, 8)))
    response_queries = draw_response_queries(jax.random.fold_in(seeds[7], 71), 0)
    response_keys = noise(seeds[4], (RESPONSES, L, DH), 1.0, 6.0, ((0, 8), (1, 32)))
    response_values = noise(seeds[5], (RESPONSES, L, DH), 3.0, 18.0, ((0, 8), (1, 32)))
    response_lengths = draw_response_lengths(jax.random.fold_in(seeds[7], 71), 0)
    return {"prompt_queries": prompt_queries, "prompt_keys": prompt_keys, "prompt_values": prompt_values, "response_queries": response_queries, "response_keys": response_keys, "response_values": response_values, "response_lengths": response_lengths}


LOWEST = -1e30


def attend(query_rows, key_rows, value_rows, allowed):
    scores = jnp.einsum("rhd,kd->rhk", query_rows.astype(jnp.float32), key_rows.astype(jnp.float32), precision=lax.Precision.HIGHEST) * (DH ** -0.5)
    masked = allowed[:, None, :]
    scores = jnp.where(masked, scores, LOWEST)
    row_max = jnp.max(scores, axis=2, keepdims=True)
    exps = jnp.where(masked, jnp.exp(scores - row_max), 0.0)
    totals = jnp.sum(exps, axis=2)
    rounded = lax.optimization_barrier(exps.astype(jnp.bfloat16))
    summed = jnp.einsum("rhk,kd->rhd", rounded.astype(jnp.float32), value_rows.astype(jnp.float32), precision=lax.Precision.HIGHEST)
    return summed / totals[:, :, None]


def reference(prompt_queries, prompt_keys, prompt_values, response_queries, response_keys, response_values, response_lengths):
    prompt_len = N_CTX * P_DEV
    prompt_grid = prompt_queries.reshape(prompt_len, HQ, DH)
    prompt_key_rows = prompt_keys.reshape(prompt_len, DH)
    prompt_value_rows = prompt_values.reshape(prompt_len, DH)
    block_width = 512 if prompt_len % 512 == 0 else prompt_len
    key_places = jnp.arange(prompt_len, dtype=jnp.int32)

    def prompt_block(block_index):
        offset = block_index * block_width
        query_rows = lax.dynamic_slice_in_dim(prompt_grid, offset, block_width, 0)
        query_places = offset + jnp.arange(block_width, dtype=jnp.int32)
        allowed = key_places[None, :] <= query_places[:, None]
        return attend(query_rows, prompt_key_rows, prompt_value_rows, allowed)

    prompt_result = lax.map(prompt_block, jnp.arange(prompt_len // block_width, dtype=jnp.int32))
    prompt_output = prompt_result.reshape(N_CTX, P_DEV, HQ * DH).astype(jnp.bfloat16)

    resp_len = N_CTX * L_DEV
    resp_width = 512 if resp_len % 512 == 0 else resp_len
    own_places = jnp.arange(resp_len, dtype=jnp.int32)

    def one_response(record):
        queries_one, keys_one, values_one, length = record
        query_grid = queries_one.reshape(resp_len, HQ, DH)
        all_keys = jnp.concatenate([prompt_key_rows, keys_one], 0)
        all_values = jnp.concatenate([prompt_value_rows, values_one], 0)

        def resp_block(block_index):
            offset = block_index * resp_width
            query_rows = lax.dynamic_slice_in_dim(query_grid, offset, resp_width, 0)
            query_places = offset + jnp.arange(resp_width, dtype=jnp.int32)
            allowed = jnp.concatenate([jnp.ones((resp_width, prompt_len), dtype=bool), own_places[None, :] <= query_places[:, None]], 1)
            result = attend(query_rows, all_keys, all_values, allowed)
            is_live = (query_places < length)[:, None, None]
            return jnp.where(is_live, result, 0.0)

        blocks = lax.map(resp_block, jnp.arange(resp_len // resp_width, dtype=jnp.int32))
        return blocks.reshape(resp_len, HQ * DH)

    response_result = lax.map(one_response, (response_queries, response_keys, response_values, response_lengths))
    return prompt_output, response_result.astype(jnp.bfloat16)
```

```python
import functools

import jax
import jax.numpy as jnp
from jax import lax
from jax.experimental import pallas as pl
from jax.experimental.pallas import tpu as pltpu
from jax.sharding import Mesh
from jax.sharding import PartitionSpec as P

DH = 128
HQ = 5
SCALE2 = DH ** (-0.5) * 1.4426950408889634
EMPTY = -1e30
MASKED = -2e30

NY, NXL, NXH, NZ, NC = 4, 2, 2, 8, 2
PR = 64
RR = 48
GR = 2
ROWS = PR + GR * RR
MP = HQ * PR
MR = HQ * RR
UNIT_AT = (0, 384, 640)
LSE_ROWS = 896
PAY = HQ * ROWS + 32
CHUNK_TILES = 2


def nt(a, b):
    return lax.dot_general(a, b, (((1,), (1,)), ((), ())), preferred_element_type=jnp.float32)


def fold(pieces, values, state):
    row_max, totals, acc = state
    top = functools.reduce(jnp.maximum, pieces)
    new_max = jnp.maximum(row_max, jnp.max(top, axis=1, keepdims=True))
    shift = new_max * SCALE2
    alpha = jnp.exp2(row_max * SCALE2 - shift)
    exps = [jnp.exp2(s * SCALE2 - shift) for s in pieces]
    total = functools.reduce(jnp.add, exps)
    totals = totals * alpha + jnp.sum(total, axis=1, keepdims=True)
    acc = acc * alpha
    for e, v in zip(exps, values):
        acc = acc + jnp.dot(e.astype(jnp.bfloat16), v, preferred_element_type=jnp.float32)
    return new_max, totals, acc


def fresh(rows):
    return (
        jnp.full((rows, 1), EMPTY, jnp.float32),
        jnp.zeros((rows, 1), jnp.float32),
        jnp.zeros((rows, DH), jnp.float32),
    )


def attend_kernel(slots, own, scal, q_ref, kva, kvb, *rest):
    if own:
        oka, okb, *rest = rest
    outs = rest[: len(slots)]
    m_s, l_s, acc_s, lse_s = rest[len(slots) :]
    y, xl, xh, z, core = (scal[i] for i in range(5))

    def piece(ref, j):
        return ref[:, j].reshape(NY * PR, 2 * DH)

    def keys_values(tiles):
        both = [piece(ref, j) for j in tiles for ref in (kva, kvb)]
        return [b[:, :DH] for b in both], [b[:, DH:] for b in both]

    def all_tiles(q, rows):
        state = fresh(rows)
        for first in range(0, NZ, CHUNK_TILES):
            keys, values = keys_values(range(first, first + CHUNK_TILES))
            state = fold([nt(q, k) for k in keys], values, state)
        return state

    def put(state, rows):
        m_s[:rows], l_s[:rows], acc_s[:rows] = state

    def get(rows):
        return m_s[:rows], l_s[:rows], acc_s[:rows]

    for n, d in enumerate(slots):
        out = outs[n]
        lse_s[...] = jnp.full(lse_s.shape, EMPTY, jnp.float32)

        def finish(unit, rows):
            m, l, acc = get(rows)
            some = l > 0.0
            o = acc / jnp.where(some, l, 1.0)
            lse = jnp.where(some, m * SCALE2 + jnp.log2(jnp.where(some, l, 1.0)), EMPTY)
            lse_s[UNIT_AT[unit] : UNIT_AT[unit] + rows] = jnp.broadcast_to(lse, (rows, DH))
            base = (0, MP, MP + MR)[unit]
            out[base : base + rows] = o.astype(jnp.bfloat16)

        def blank(unit, rows):
            base = (0, MP, MP + MR)[unit]
            out[base : base + rows] = jnp.zeros((rows, DH), jnp.bfloat16)

        qp = q_ref[d, :, :PR].reshape(MP, DH)
        if d & 1:

            @pl.when(xh == 0)
            def _():
                put(all_tiles(qp, MP), MP)
                finish(0, MP)

            @pl.when(xh != 0)
            def _():
                blank(0, MP)
        else:
            xl_d = jnp.bitwise_xor(xl, d >> 1)
            row = lax.broadcasted_iota(jnp.int32, (MP, 1), 0) % PR
            q_at = core * 512 + y * 128 + xl_d * PR + row
            col = lax.broadcasted_iota(jnp.int32, (1, NY * PR), 1)
            k_at = (col // PR) * 128 + xl * PR + col % PR
            put(fresh(MP), MP)
            for first in range(0, NZ, CHUNK_TILES):

                @pl.when(z >= first)
                def _():
                    tiles = range(first, first + CHUNK_TILES)
                    keys, values = keys_values(tiles)
                    parts = [((j - z) * 1024 + c * 512) for j in tiles for c in (core, 1 - core)]
                    pieces = [
                        jnp.where(k_at + at <= q_at, nt(qp, k), MASKED) for at, k in zip(parts, keys)
                    ]
                    put(fold(pieces, values, get(MP)), MP)

            finish(0, MP)

        for g in range(GR):
            live = scal[5 + d * GR + g]

            @pl.when(live != 0)
            def _():
                qr = q_ref[d, :, PR + g * RR : PR + (g + 1) * RR].reshape(MR, DH)
                put(all_tiles(qr, MR), MR)
                if own:
                    xh_d = jnp.bitwise_xor(xh, d & 1)

                    @pl.when(xh_d >= xh)
                    def _():
                        row = lax.broadcasted_iota(jnp.int32, (MR, 1), 0) % RR
                        q_at = (xh_d - xh) * (16 * RR) + (2 * z + core) * RR + row
                        width = NZ * RR
                        col = lax.broadcasted_iota(jnp.int32, (1, width), 1)
                        k_at = (col // RR) * (2 * RR) + col % RR
                        pieces, values = [], []
                        for ref, c in ((oka, core), (okb, 1 - core)):
                            both = ref[:, g].reshape(width, 2 * DH)
                            s = nt(qr, both[:, :DH])
                            pieces.append(jnp.where(k_at + c * RR <= q_at, s, MASKED))
                            values.append(both[:, DH:])
                        put(fold(pieces, values, get(MR)), MR)

                finish(1 + g, MR)

            @pl.when(live == 0)
            def _():
                blank(1 + g, MR)

        eye = lax.broadcasted_iota(jnp.int32, (DH, DH), 0) == lax.broadcasted_iota(
            jnp.int32, (DH, DH), 1
        )
        lse = [
            jnp.sum(jnp.where(eye, lse_s[b * DH : (b + 1) * DH], 0.0), axis=0, keepdims=True)
            for b in range(LSE_ROWS // DH)
        ]
        lse = jnp.concatenate(lse + [jnp.zeros((1, DH), jnp.float32)], axis=0)
        hi = lse.astype(jnp.bfloat16).astype(jnp.float32)
        mid = (lse - hi).astype(jnp.bfloat16).astype(jnp.float32)
        low = lse - hi - mid
        parts = jnp.concatenate([hi, mid, low, jnp.zeros_like(low)], axis=0)
        out[HQ * ROWS :] = parts.astype(jnp.bfloat16)


def attend(slots, own, scal, q, *arrays):
    vmem = pl.BlockSpec(memory_space=pltpu.VMEM)
    return pl.pallas_call(
        functools.partial(attend_kernel, slots, own),
        in_specs=[pl.BlockSpec(memory_space=pltpu.SMEM)] + [vmem] * (1 + len(arrays)),
        out_specs=[vmem] * len(slots),
        out_shape=[jax.ShapeDtypeStruct((PAY, DH), jnp.bfloat16)] * len(slots),
        scratch_shapes=[
            pltpu.VMEM((MP, 1), jnp.float32),
            pltpu.VMEM((MP, 1), jnp.float32),
            pltpu.VMEM((MP, DH), jnp.float32),
            pltpu.VMEM((LSE_ROWS, DH), jnp.float32),
        ],
        compiler_params=pltpu.CompilerParams(vmem_limit_bytes=48 * 1024 * 1024),
        name="attend_own" if own else "attend",
    )(scal, q, *arrays)


def merge_kernel(live, p0, p1, p2, p3, prompt_out, response_out):
    parts = (p0, p1, p2, p3)
    lses = []
    for p in parts:
        t = p[HQ * ROWS :].astype(jnp.float32)
        lses.append(t[0:8] + t[8:16] + t[16:24])
    top = functools.reduce(jnp.maximum, lses)
    weights = [jnp.exp2(s - top) for s in lses]
    total = functools.reduce(jnp.add, weights)
    weights = [w / total for w in weights]
    stack = jnp.concatenate(weights + [jnp.zeros((DH - 32, DH), jnp.float32)], axis=0)
    cols = jnp.transpose(stack)

    def unit(base, rows, at):
        pieces = []
        for b0 in range(0, rows, DH):
            height = min(DH, rows - b0)
            block = (at + b0) // DH
            acc = None
            for n, p in enumerate(parts):
                w = cols[:height, n * 8 + block : n * 8 + block + 1]
                term = p[base + b0 : base + b0 + height].astype(jnp.float32) * w
                acc = term if acc is None else acc + term
            pieces.append(acc)
        return jnp.concatenate(pieces, axis=0)

    o = unit(0, MP, UNIT_AT[0])
    for h in range(HQ):
        prompt_out[:, h * DH : (h + 1) * DH] = o[h * PR : (h + 1) * PR].astype(jnp.bfloat16)
    row = lax.broadcasted_iota(jnp.int32, (RR, 1), 0)
    for g in range(GR):
        o = unit(MP + g * MR, MR, UNIT_AT[1 + g])
        keep = row < live[g]
        for h in range(HQ):
            response_out[g, :, h * DH : (h + 1) * DH] = jnp.where(
                keep, o[h * RR : (h + 1) * RR], 0.0
            ).astype(jnp.bfloat16)


def merge(live, *parts):
    vmem = pl.BlockSpec(memory_space=pltpu.VMEM)
    return pl.pallas_call(
        merge_kernel,
        in_specs=[pl.BlockSpec(memory_space=pltpu.SMEM)] + [vmem] * 4,
        out_specs=[vmem] * 2,
        out_shape=[
            jax.ShapeDtypeStruct((PR, HQ * DH), jnp.bfloat16),
            jax.ShapeDtypeStruct((GR, RR, HQ * DH), jnp.bfloat16),
        ],
        name="merge",
    )(live, *parts)


def flip_x(value, d):
    return lax.ppermute(value, ("xl", "xh"), [(s, s ^ d) for s in range(NXL * NXH)])


def flip_core(value):
    return lax.ppermute(value, "core", [(0, 1), (1, 0)])


def copy_for_each(value, axes, count):
    many = jnp.broadcast_to(value[None], (count, *value.shape))
    return lax.all_to_all(many, axes, 0, 0, tiled=True)


def shards(
    prompt_queries,
    prompt_keys,
    prompt_values,
    response_queries,
    response_keys,
    response_values,
    response_lengths,
):
    y, xl, xh, z, core = (lax.axis_index(a).astype(jnp.int32) for a in ("y", "xl", "xh", "z", "core"))

    prompt_kv = jnp.concatenate([prompt_keys[0], prompt_values[0]], axis=1)
    kv_a = copy_for_each(prompt_kv, ("y", "z"), NY * NZ).reshape(NY, NZ, PR, 2 * DH)

    queries = jnp.concatenate([prompt_queries[0], response_queries.reshape(GR * RR, HQ * DH)], axis=0)
    gathered = [queries] + [flip_x(queries, d) for d in (1, 2, 3)]
    q = jnp.stack(gathered).reshape(4, ROWS, HQ, DH).transpose(0, 2, 1, 3)
    other_lengths = lax.ppermute(response_lengths, "xl", [(0, 1), (1, 0)])

    kv_b = flip_core(kv_a)
    own_kv = jnp.concatenate([response_keys, response_values], axis=2)
    own_a = copy_for_each(own_kv, "z", NZ)
    own_b = flip_core(own_a)

    block = 2 * z + core
    lengths = jnp.stack([response_lengths, response_lengths, other_lengths, other_lengths])
    blocks = jnp.stack([xh, 1 - xh, xh, 1 - xh]) * 16 + block
    is_live = (blocks[:, None] * RR < lengths).astype(jnp.int32)
    scal = jnp.concatenate([jnp.stack([y, xl, xh, z, core]), is_live.reshape(-1)])

    pay2, pay3 = attend((2, 3), False, scal, q, kv_a, kv_b)
    got2, got3 = flip_x(pay2, 2), flip_x(pay3, 3)
    pay1, pay0 = attend((1, 0), True, scal, q, kv_a, kv_b, own_a, own_b)
    got1 = flip_x(pay1, 1)
    live_rows = response_lengths - (xh * 16 + block) * RR
    prompt_out, response_out = merge(live_rows, pay0, got1, got2, got3)
    return prompt_out[None], response_out


def solution(mesh):
    fine = Mesh(mesh.devices.reshape(NY, NXL, NXH, NZ, NC), ("y", "xl", "xh", "z", "core"))
    resp, ctx = ("y", "xl"), ("xh", "z", "core")
    in_specs = (
        P(ctx, resp, None),
        P(ctx, resp, None),
        P(ctx, resp, None),
        P(resp, ctx, None),
        P(resp, ctx, None),
        P(resp, ctx, None),
        P(resp),
    )
    out_specs = (P(ctx, resp, None), P(resp, ctx, None))
    return jax.shard_map(shards, mesh=fine, in_specs=in_specs, out_specs=out_specs, check_vma=False)
```

```python
import functools

import jax
import jax.numpy as jnp
from jax import lax
from jax.experimental import pallas as pl
from jax.experimental.pallas import tpu as pltpu
from jax.sharding import Mesh
from jax.sharding import PartitionSpec as P

DH = 128
HQ = 5
SCALE2 = DH ** (-0.5) * 1.4426950408889634
EMPTY = -1e30
MASKED = -2e30

NY, NXL, NXH, NZ, NC = 4, 2, 2, 8, 2
PR = 64
RR = 48
GR = 2
ROWS = PR + GR * RR
MP = HQ * PR
MR = HQ * RR
UNIT_AT = (0, 384, 640)
LSE_ROWS = 896
PAY = HQ * ROWS + 32
CHUNK_TILES = 2


def nt(a, b):
    return lax.dot_general(a, b, (((1,), (1,)), ((), ())), preferred_element_type=jnp.float32)


def heads(q_ref, first, rows):
    return jnp.concatenate(
        [q_ref[first : first + rows, h * DH : (h + 1) * DH] for h in range(HQ)], axis=0
    )


def plain(q, blocks, state):
    totals, acc = state
    total = None
    for keys, values, mask in blocks:
        e = jnp.exp2(nt(q, keys) * SCALE2)
        if mask is not None:
            e = jnp.where(mask, e, 0.0)
        total = e if total is None else total + e
        acc = acc + jnp.dot(e.astype(jnp.bfloat16), values, preferred_element_type=jnp.float32)
    return totals + jnp.sum(total, axis=1, keepdims=True), acc


def fold(pieces, values, state):
    row_max, totals, acc = state
    top = functools.reduce(jnp.maximum, [jnp.max(s, axis=1, keepdims=True) for s in pieces])
    new_max = jnp.maximum(row_max, top)
    shift = new_max * SCALE2
    alpha = jnp.exp2(row_max * SCALE2 - shift)
    totals, acc = totals * alpha, acc * alpha
    for s, v in zip(pieces, values):
        e = jnp.exp2(s * SCALE2 - shift)
        totals = totals + jnp.sum(e, axis=1, keepdims=True)
        acc = acc + jnp.dot(e.astype(jnp.bfloat16), v, preferred_element_type=jnp.float32)
    return new_max, totals, acc


def fresh(rows):
    return jnp.zeros((rows, 1), jnp.float32), jnp.zeros((rows, DH), jnp.float32)


def split(both):
    return both[:, :DH], both[:, DH:]


def own_mask(xh, xh_d, z, core, part):
    row = lax.broadcasted_iota(jnp.int32, (MR, 1), 0) % RR
    q_at = (xh_d - xh) * (16 * RR) + (2 * z + core) * RR + row
    col = lax.broadcasted_iota(jnp.int32, (1, NZ * RR), 1)
    return (col // RR) * (2 * RR) + col % RR + part * RR <= q_at


UNITS = ((0, MP), (MP, MR), (MP + MR, MR))


def first_kernel(scal, q0, q1, q2, q3, zkv_a, zkv_b, l_out, acc_out):
    y, xl, xh, z, core = (scal[i] for i in range(5))

    def column(q, state):
        blocks = []
        for first in range(0, NZ, 4):
            for ref in (zkv_a, zkv_b):
                keys, values = split(ref[first : first + 4, :PR].reshape(4 * PR, 2 * DH))
                blocks.append((keys, values, None))
        return plain(q, blocks, state)

    for d, q_ref in ((3, q3), (1, q1)):

        @pl.when(xh == 0)
        def _():
            l_out[d, :MP], acc_out[d, :MP] = column(heads(q_ref, 0, PR), fresh(MP))

    for d, q_ref in ((3, q3), (2, q2), (1, q1), (0, q0)):
        for g in range(GR):
            base, rows = UNITS[1 + g]

            @pl.when(scal[5 + d * GR + g] != 0)
            def _():
                q = heads(q_ref, PR + g * RR, RR)
                l_out[d, base : base + rows], acc_out[d, base : base + rows] = column(q, fresh(rows))
                if d < 2:
                    xh_d = jnp.bitwise_xor(xh, d)

                    @pl.when(xh_d >= xh)
                    def _():
                        state = l_out[d, base : base + rows], acc_out[d, base : base + rows]
                        for ref, part in ((zkv_a, core), (zkv_b, 1 - core)):
                            own = ref[:, PR + g * RR : PR + (g + 1) * RR].reshape(NZ * RR, 2 * DH)
                            keys, values = split(own)
                            mask = own_mask(xh, xh_d, z, core, part)
                            state = plain(q, [(keys, values, mask)], state)
                        l_out[d, base : base + rows], acc_out[d, base : base + rows] = state


def attend_kernel(slots, scal, *refs):
    n = len(slots)
    q_refs, (l_in, acc_in, zkv_a, zkv_b, ykv_a, ykv_b) = refs[:n], refs[n : n + 6]
    outs, (m_s, l_s, acc_s, lse_s, bad_s) = refs[n + 6 : 2 * n + 6], refs[2 * n + 6 :]
    y, xl, xh, z, core = (scal[i] for i in range(5))
    bad_s[...] = jnp.zeros(bad_s.shape, jnp.float32)

    def others(q, state):
        blocks = []
        for step in range(1, NY):
            yy = lax.rem(y + step, NY)
            for first in range(0, NZ, 4):
                for ref in (ykv_a, ykv_b):
                    keys, values = split(ref[yy, first : first + 4].reshape(4 * PR, 2 * DH))
                    blocks.append((keys, values, None))
        return plain(q, blocks, state)

    def q_position(d):
        row = lax.broadcasted_iota(jnp.int32, (MP, 1), 0) % PR
        xl_d = jnp.bitwise_xor(xl, d >> 1)
        return (2 * z + core) * 512 + y * 128 + xl_d * PR + row

    def k_position(zz, part, width):
        col = lax.broadcasted_iota(jnp.int32, (1, width), 1)
        return (2 * zz + part) * 512 + (col // PR) * 128 + xl * PR + col % PR

    def finish(slot, unit, m, l, acc, needed):
        some = l > 0.0
        safe = jnp.where(some, l, 1.0)
        o = acc / safe
        lse = jnp.log2(safe) if m is None else m * SCALE2 + jnp.log2(safe)
        lse = jnp.where(some, lse, EMPTY)
        base, rows = UNITS[unit]
        outs[slot][base : base + rows] = o.astype(jnp.bfloat16)
        lse_s[slot, UNIT_AT[unit] : UNIT_AT[unit] + rows] = jnp.broadcast_to(lse, (rows, DH))
        if m is None:
            good = (l >= 2.0**-40) & (l <= 2.0**100)
            if needed is not None:
                good = good | jnp.logical_not(needed)
            bad_s[:rows] = jnp.maximum(bad_s[:rows], jnp.where(good, 0.0, 1.0))

    def blank(slot, unit):
        base, rows = UNITS[unit]
        outs[slot][base : base + rows] = jnp.zeros((rows, DH), jnp.bfloat16)
        lse_s[slot, UNIT_AT[unit] : UNIT_AT[unit] + rows] = jnp.full((rows, DH), EMPTY, jnp.float32)

    for slot, d in enumerate(slots):
        for at, width in ((320, 64), (624, 16), (880, 16)):
            lse_s[slot, at : at + width] = jnp.full((width, DH), EMPTY, jnp.float32)
        if d & 1:

            @pl.when(xh == 0)
            def _():
                q = heads(q_refs[slot], 0, PR)
                l, acc = others(q, (l_in[d, :MP], acc_in[d, :MP]))
                finish(slot, 0, None, l, acc, None)

            @pl.when(xh != 0)
            def _():
                blank(slot, 0)
        else:
            q_at = q_position(d)
            l_s[...], acc_s[...] = fresh(MP)
            for first in range(0, NZ, 2):

                @pl.when(z >= first)
                def _():
                    q = heads(q_refs[slot], 0, PR)
                    blocks = []
                    for zz in (first, first + 1):
                        for ref, part in ((ykv_a, core), (ykv_b, 1 - core)):
                            keys, values = split(ref[:, zz].reshape(NY * PR, 2 * DH))
                            blocks.append((keys, values, k_position(zz, part, NY * PR) <= q_at))
                    l_s[...], acc_s[...] = plain(q, blocks, (l_s[...], acc_s[...]))

            finish(slot, 0, None, l_s[...], acc_s[...], q_at >= xl * PR)
        for g in range(GR):
            base, rows = UNITS[1 + g]
            live = scal[5 + d * GR + g]

            @pl.when(live != 0)
            def _():
                q = heads(q_refs[slot], PR + g * RR, RR)
                l, acc = others(q, (l_in[d, base : base + rows], acc_in[d, base : base + rows]))
                finish(slot, 1 + g, None, l, acc, None)

            @pl.when(live == 0)
            def _():
                blank(slot, 1 + g)

    @pl.when(jnp.max(bad_s[...]) > 0.0)
    def _():
        for slot, d in enumerate(slots):
            for unit in range(3):
                base, rows = UNITS[unit]
                xh_d = jnp.bitwise_xor(xh, d & 1)
                if unit == 0:
                    active = xh_d >= xh
                else:
                    active = scal[5 + d * GR + unit - 1] != 0

                @pl.when(active)
                def _():
                    if unit == 0:
                        q = heads(q_refs[slot], 0, PR)
                        q_at = q_position(d) + (xh_d - xh) * (16 * 512)
                    else:
                        q = heads(q_refs[slot], PR + (unit - 1) * RR, RR)
                    m_s[:rows] = jnp.full((rows, 1), EMPTY, jnp.float32)
                    l_s[:rows], acc_s[:rows] = fresh(rows)

                    def put(pieces, values):
                        m_s[:rows], l_s[:rows], acc_s[:rows] = fold(
                            pieces, values, (m_s[:rows], l_s[:rows], acc_s[:rows])
                        )

                    @pl.loop(0, NZ)
                    def _(zz):
                        for ref, part in ((ykv_a, core), (ykv_b, 1 - core)):
                            keys, values = split(ref[:, zz].reshape(NY * PR, 2 * DH))
                            s = nt(q, keys)
                            if unit == 0:
                                s = jnp.where(k_position(zz, part, NY * PR) <= q_at, s, MASKED)
                            put([s], [values])

                    if unit > 0 and d < 2:

                        @pl.when(xh_d >= xh)
                        def _():
                            for ref, part in ((zkv_a, core), (zkv_b, 1 - core)):
                                first = PR + (unit - 1) * RR
                                own = ref[:, first : first + RR].reshape(NZ * RR, 2 * DH)
                                keys, values = split(own)
                                mask = own_mask(xh, xh_d, z, core, part)
                                put([jnp.where(mask, nt(q, keys), MASKED)], [values])

                    finish(slot, unit, m_s[:rows], l_s[:rows], acc_s[:rows], None)

    eye = lax.broadcasted_iota(jnp.int32, (DH, DH), 0) == lax.broadcasted_iota(
        jnp.int32, (DH, DH), 1
    )
    for slot in range(n):
        lse = [
            jnp.sum(jnp.where(eye, lse_s[slot, b * DH : (b + 1) * DH], 0.0), axis=0, keepdims=True)
            for b in range(LSE_ROWS // DH)
        ]
        lse = jnp.concatenate(lse + [jnp.zeros((1, DH), jnp.float32)], axis=0)
        hi = lse.astype(jnp.bfloat16).astype(jnp.float32)
        mid = (lse - hi).astype(jnp.bfloat16).astype(jnp.float32)
        low = lse - hi - mid
        parts = jnp.concatenate([hi, mid, low, jnp.zeros_like(low)], axis=0)
        outs[slot][HQ * ROWS :] = parts.astype(jnp.bfloat16)


VMEM = pl.BlockSpec(memory_space=pltpu.VMEM)
SMEM = pl.BlockSpec(memory_space=pltpu.SMEM)


def first_stage(scal, qs, zkv_a, zkv_b):
    return pl.pallas_call(
        first_kernel,
        in_specs=[SMEM] + [VMEM] * 6,
        out_specs=[VMEM] * 2,
        out_shape=[
            jax.ShapeDtypeStruct((4, HQ * ROWS, 1), jnp.float32),
            jax.ShapeDtypeStruct((4, HQ * ROWS, DH), jnp.float32),
        ],
        compiler_params=pltpu.CompilerParams(vmem_limit_bytes=48 * 1024 * 1024),
        cost_estimate=pl.CostEstimate(flops=4_000_000_000, transcendentals=0, bytes_accessed=0),
        name="first",
    )(scal, *qs, zkv_a, zkv_b)


def attend(slots, scal, qs, *arrays):
    return pl.pallas_call(
        functools.partial(attend_kernel, slots),
        in_specs=[SMEM] + [VMEM] * (len(slots) + 6),
        out_specs=[VMEM] * len(slots),
        out_shape=[jax.ShapeDtypeStruct((PAY, DH), jnp.bfloat16)] * len(slots),
        scratch_shapes=[
            pltpu.VMEM((MP, 1), jnp.float32),
            pltpu.VMEM((MP, 1), jnp.float32),
            pltpu.VMEM((MP, DH), jnp.float32),
            pltpu.VMEM((len(slots), LSE_ROWS, DH), jnp.float32),
            pltpu.VMEM((MP, 1), jnp.float32),
        ],
        compiler_params=pltpu.CompilerParams(vmem_limit_bytes=48 * 1024 * 1024),
        cost_estimate=pl.CostEstimate(
            flops=2_000_000_000 * len(slots), transcendentals=0, bytes_accessed=0
        ),
        name="attend" + "".join(map(str, slots)),
    )(scal, *[qs[d] for d in slots], *arrays)


def merge_kernel(live, p0, p1, p2, p3, prompt_out, response_out):
    parts = (p0, p1, p2, p3)
    lses = []
    for p in parts:
        t = p[HQ * ROWS :].astype(jnp.float32)
        lses.append(t[0:8] + t[8:16] + t[16:24])
    top = functools.reduce(jnp.maximum, lses)
    weights = [jnp.exp2(s - top) for s in lses]
    total = functools.reduce(jnp.add, weights)
    weights = [w / total for w in weights]
    stack = jnp.concatenate(weights + [jnp.zeros((DH - 32, DH), jnp.float32)], axis=0)
    cols = jnp.transpose(stack)

    def unit(base, rows, at):
        pieces = []
        for b0 in range(0, rows, DH):
            height = min(DH, rows - b0)
            block = (at + b0) // DH
            acc = None
            for n, p in enumerate(parts):
                w = cols[:height, n * 8 + block : n * 8 + block + 1]
                term = p[base + b0 : base + b0 + height].astype(jnp.float32) * w
                acc = term if acc is None else acc + term
            pieces.append(acc)
        return jnp.concatenate(pieces, axis=0)

    o = unit(0, MP, UNIT_AT[0])
    for h in range(HQ):
        prompt_out[:, h * DH : (h + 1) * DH] = o[h * PR : (h + 1) * PR].astype(jnp.bfloat16)
    row = lax.broadcasted_iota(jnp.int32, (RR, 1), 0)
    for g in range(GR):
        o = unit(MP + g * MR, MR, UNIT_AT[1 + g])
        keep = row < live[g]
        for h in range(HQ):
            response_out[g, :, h * DH : (h + 1) * DH] = jnp.where(
                keep, o[h * RR : (h + 1) * RR], 0.0
            ).astype(jnp.bfloat16)


def merge(live, *parts):
    vmem = pl.BlockSpec(memory_space=pltpu.VMEM)
    return pl.pallas_call(
        merge_kernel,
        in_specs=[pl.BlockSpec(memory_space=pltpu.SMEM)] + [vmem] * 4,
        out_specs=[vmem] * 2,
        out_shape=[
            jax.ShapeDtypeStruct((PR, HQ * DH), jnp.bfloat16),
            jax.ShapeDtypeStruct((GR, RR, HQ * DH), jnp.bfloat16),
        ],
        name="merge",
    )(live, *parts)


def flip_x(value, d):
    return lax.ppermute(value, ("xl", "xh"), [(s, s ^ d) for s in range(NXL * NXH)])


def flip_core(value):
    return lax.ppermute(value, "core", [(0, 1), (1, 0)])


def copy_for_each(value, axes, count):
    many = jnp.broadcast_to(value[None], (count, *value.shape))
    return lax.all_to_all(many, axes, 0, 0, tiled=True)


def shards(
    prompt_queries,
    prompt_keys,
    prompt_values,
    response_queries,
    response_keys,
    response_values,
    response_lengths,
):
    y, xl, xh, z, core = (lax.axis_index(a).astype(jnp.int32) for a in ("y", "xl", "xh", "z", "core"))

    queries = jnp.concatenate([prompt_queries[0], response_queries.reshape(GR * RR, HQ * DH)], axis=0)
    keys = jnp.concatenate([prompt_keys[0], response_keys.reshape(GR * RR, DH)], axis=0)
    values = jnp.concatenate([prompt_values[0], response_values.reshape(GR * RR, DH)], axis=0)
    zkv_a = copy_for_each(jnp.concatenate([keys, values], axis=1), "z", NZ)
    qs = [queries] + [flip_x(queries, d) for d in (1, 2, 3)]
    other_lengths = lax.ppermute(response_lengths, "xl", [(0, 1), (1, 0)])

    block = 2 * z + core
    lengths = jnp.stack([response_lengths, response_lengths, other_lengths, other_lengths])
    blocks = jnp.stack([xh, 1 - xh, xh, 1 - xh]) * 16 + block
    is_live = (blocks[:, None] * RR < lengths).astype(jnp.int32)
    scal = jnp.concatenate([jnp.stack([y, xl, xh, z, core]), is_live.reshape(-1)])

    zkv_a, scal, *qs = lax.optimization_barrier((zkv_a, scal, *qs))
    ykv_a = copy_for_each(zkv_a[:, :PR], "y", NY)
    zkv_b = flip_core(zkv_a)
    state = first_stage(scal, qs, zkv_a, zkv_b)
    ykv_a, *state = lax.optimization_barrier((ykv_a, *state))
    ykv_b = flip_core(ykv_a)

    arrays = (*state, zkv_a, zkv_b, ykv_a, ykv_b)
    pay3, pay2 = attend((3, 2), scal, qs, *arrays)
    got3, got2 = flip_x(pay3, 3), flip_x(pay2, 2)
    scal, pay3 = lax.optimization_barrier((scal, pay3))
    (pay1,) = attend((1,), scal, qs, *arrays)
    got1 = flip_x(pay1, 1)
    scal, pay1 = lax.optimization_barrier((scal, pay1))
    (pay0,) = attend((0,), scal, qs, *arrays)
    live_rows = response_lengths - (xh * 16 + block) * RR
    prompt_out, response_out = merge(live_rows, pay0, got1, got2, got3)
    return prompt_out[None], response_out


def solution(mesh):
    fine = Mesh(mesh.devices.reshape(NY, NXL, NXH, NZ, NC), ("y", "xl", "xh", "z", "core"))
    resp, ctx = ("y", "xl"), ("xh", "z", "core")
    in_specs = (
        P(ctx, resp, None),
        P(ctx, resp, None),
        P(ctx, resp, None),
        P(resp, ctx, None),
        P(resp, ctx, None),
        P(resp, ctx, None),
        P(resp),
    )
    out_specs = (P(ctx, resp, None), P(resp, ctx, None))
    return jax.shard_map(shards, mesh=fine, in_specs=in_specs, out_specs=out_specs, check_vma=False)
```

```python
import functools

import jax
import jax.numpy as jnp
from jax import lax
from jax.experimental import pallas as pl
from jax.experimental.pallas import tpu as pltpu
from jax.sharding import Mesh
from jax.sharding import PartitionSpec as P

DH = 128
HQ = 5
SCALE2 = DH ** (-0.5) * 1.4426950408889634
EMPTY = -1e30
MASKED = -2e30

NY, NXL, NXH, NZ, NC = 4, 2, 2, 8, 2
PR = 64
RR = 48
GR = 2
ROWS = PR + GR * RR
MP = HQ * PR
MR = HQ * RR
UNIT_AT = (0, 384, 640)
LSE_ROWS = 896
PAY = HQ * ROWS + 32
GRANT = 16 * 1024 * 1024


def nt(a, b):
    return lax.dot_general(a, b, (((1,), (1,)), ((), ())), preferred_element_type=jnp.float32)


def heads(q_ref, first, rows):
    return jnp.concatenate(
        [q_ref[first : first + rows, h * DH : (h + 1) * DH] for h in range(HQ)], axis=0
    )


def plain(q, blocks, state):
    totals, acc = state
    exps, values, total = [], [], None
    for both, mask in blocks:
        keys, value = split(both)
        e = jnp.exp2(nt(q, keys) * SCALE2)
        if mask is not None:
            e = jnp.where(mask, e, 0.0)
        for at in range(0, e.shape[1], DH):
            part = e[:, at : at + DH]
            total = part if total is None else total + part
        exps.append(e.astype(jnp.bfloat16))
        values.append(value)
    exps, values = jnp.concatenate(exps, axis=1), jnp.concatenate(values, axis=0)
    acc = acc + jnp.dot(exps, values, preferred_element_type=jnp.float32)
    return totals + jnp.sum(total, axis=1, keepdims=True), acc


def fold(pieces, values, state):
    row_max, totals, acc = state
    top = functools.reduce(jnp.maximum, [jnp.max(s, axis=1, keepdims=True) for s in pieces])
    new_max = jnp.maximum(row_max, top)
    shift = new_max * SCALE2
    alpha = jnp.exp2(row_max * SCALE2 - shift)
    totals, acc = totals * alpha, acc * alpha
    for s, v in zip(pieces, values):
        e = jnp.exp2(s * SCALE2 - shift)
        totals = totals + jnp.sum(e, axis=1, keepdims=True)
        acc = acc + jnp.dot(e.astype(jnp.bfloat16), v, preferred_element_type=jnp.float32)
    return new_max, totals, acc


def fresh(rows):
    return jnp.zeros((rows, 1), jnp.float32), jnp.zeros((rows, DH), jnp.float32)


def split(both):
    return both[:, :DH], both[:, DH:]


def own_mask(xh, xh_d, z, core, part):
    row = lax.broadcasted_iota(jnp.int32, (MR, 1), 0) % RR
    q_at = (xh_d - xh) * (16 * RR) + (2 * z + core) * RR + row
    col = lax.broadcasted_iota(jnp.int32, (1, NZ * RR), 1)
    return (col // RR) * (2 * RR) + col % RR + part * RR <= q_at


UNITS = ((0, MP), (MP, MR), (MP + MR, MR))
HALF = NZ // 2


def rows_of(block):
    return block.reshape(block.shape[0] * block.shape[1], 2 * DH)


def whole(ref_a, ref_b, step):
    return step, [
        [lambda r=r, h=h: rows_of(r[h * HALF : (h + 1) * HALF]) for r in (ref_a, ref_b)]
        for h in range(2)
    ]


def halves(low_a, low_b, high_a, high_b, step):
    return step, [[lambda r=r: rows_of(r[...]) for r in pair] for pair in ((low_a, low_b), (high_a, high_b))]


class Place:
    def __init__(self, scal):
        self.scal = scal
        self.y, self.xl, self.xh, self.z, self.core = (scal[i] for i in range(5))

    def live(self, d, g):
        return self.scal[5 + d * GR + g]

    def other_xh(self, d):
        return jnp.bitwise_xor(self.xh, d & 1)

    def query_at(self, d):
        row = lax.broadcasted_iota(jnp.int32, (MP, 1), 0) % PR
        xl_d = jnp.bitwise_xor(self.xl, d >> 1)
        return (2 * self.z + self.core) * 512 + self.y * 128 + xl_d * PR + row

    def key_at(self, step, first, part, width):
        col = lax.broadcasted_iota(jnp.int32, (1, width), 1)
        yy = lax.rem(self.y + step, NY)
        return (2 * (first + col // PR) + part) * 512 + yy * 128 + self.xl * PR + col % PR


def all_keys(q, sources, state):
    for _, parts in sources:
        state = plain(q, [(get(), None) for half in parts for get in half], state)
    return state


def diagonal(place, d, q_of, sources, load, store):
    q_at = place.query_at(d)
    for h in range(2):

        @pl.when(place.z >= h * HALF)
        def _():
            state = load()
            q = q_of()
            for step, parts in sources:
                blocks = []
                for get, part in zip(parts[h], (place.core, 1 - place.core)):
                    mask = place.key_at(step, h * HALF, part, HALF * PR) <= q_at
                    blocks.append((get(), mask))
                state = plain(q, blocks, state)
            store(state)


def column(d, unit):
    return 3 * d + unit


def get_total(ref, d, unit, rows):
    at = column(d, unit)
    return ref[:rows, at : at + 1]


def put_total(ref, d, unit, rows, total):
    lane = lax.broadcasted_iota(jnp.int32, (rows, DH), 1)
    ref[:rows] = jnp.where(lane == column(d, unit), total, ref[:rows])


def stage_kernel(slots, steps, later, scal, *refs):
    n = len(slots)
    q_refs, refs = refs[:n], refs[n:]
    if later:
        l_in, *refs = refs
        acc_in, refs = refs[:n], refs[n:]
    sources = [whole(refs[2 * i], refs[2 * i + 1], step) for i, step in enumerate(steps)]
    l_out, *acc_out = refs[2 * len(steps) :]
    l_out[...] = l_in[...] if later else jnp.zeros(l_out.shape, jnp.float32)
    place = Place(scal)
    for slot, d in enumerate(slots):

        def start(unit):
            base, rows = UNITS[unit]
            if later:
                return get_total(l_in, d, unit, rows), acc_in[slot][base : base + rows]
            return fresh(rows)

        def store(unit, state):
            base, rows = UNITS[unit]
            put_total(l_out, d, unit, rows, state[0])
            acc_out[slot][base : base + rows] = state[1]

        if d & 1:

            @pl.when(place.xh == 0)
            def _():
                store(0, all_keys(heads(q_refs[slot], 0, PR), sources, start(0)))
        else:
            store(0, start(0))
            diagonal(
                place,
                d,
                lambda: heads(q_refs[slot], 0, PR),
                sources,
                lambda: (get_total(l_out, d, 0, MP), acc_out[slot][:MP]),
                lambda state: store(0, state),
            )
        for g in range(GR):

            @pl.when(place.live(d, g) != 0)
            def _():
                q = heads(q_refs[slot], PR + g * RR, RR)
                store(1 + g, all_keys(q, sources, start(1 + g)))


def attend_kernel(slots, more, scal, *refs):
    n, k = len(slots), 4 if more else 0
    q_refs, refs = refs[:n], refs[n:]
    l_in, *refs = refs
    acc_in, near, refs = refs[:n], refs[n : n + k], refs[n + k :]
    (la, lb, ha, hb, oa, ob), far, refs = refs[:6], refs[6:12], refs[12:]
    outs, (m_s, l_s, acc_s, lse_s, bad_s, far_s, sems) = refs[:n], refs[n:]
    place = Place(scal)
    xh, z, core = place.xh, place.z, place.core
    sources = [halves(la, lb, ha, hb, 2)]
    if more:
        sources = [whole(*near[:2], NY - 1), whole(*near[2:], 1)] + sources
    bad_s[...] = jnp.zeros(bad_s.shape, jnp.float32)

    def own_blocks(d, g):
        blocks = []
        for ref, part in ((oa, core), (ob, 1 - core)):
            mask = own_mask(xh, place.other_xh(d), z, core, part)
            blocks.append((rows_of(ref[:, g]), mask))
        return blocks

    def finish(slot, unit, first, m, l, acc, needed):
        some = l > 0.0
        safe = jnp.where(some, l, 1.0)
        o = acc / safe
        lse = jnp.log2(safe) if m is None else m * SCALE2 + jnp.log2(safe)
        lse = jnp.where(some, lse, EMPTY)
        rows = l.shape[0]
        first = first if isinstance(first, int) else pl.multiple_of(first, 16)
        outs[slot][pl.ds(UNITS[unit][0] + first, rows)] = o.astype(jnp.bfloat16)
        lse_s[slot, pl.ds(UNIT_AT[unit] + first, rows)] = jnp.broadcast_to(lse, (rows, DH))
        if m is None:
            good = (l >= 2.0**-40) & (l <= 2.0**100)
            if needed is not None:
                good = good | jnp.logical_not(needed)
            bad_s[:rows] = jnp.maximum(bad_s[:rows], jnp.where(good, 0.0, 1.0))

    def blank(slot, unit):
        base, rows = UNITS[unit]
        outs[slot][base : base + rows] = jnp.zeros((rows, DH), jnp.bfloat16)
        lse_s[slot, UNIT_AT[unit] : UNIT_AT[unit] + rows] = jnp.full((rows, DH), EMPTY, jnp.float32)

    for slot, d in enumerate(slots):

        def start(unit):
            base, rows = UNITS[unit]
            return get_total(l_in, d, unit, rows), acc_in[slot][base : base + rows]

        for gap, width in ((320, 64), (624, 16), (880, 16)):
            lse_s[slot, gap : gap + width] = jnp.full((width, DH), EMPTY, jnp.float32)
        if d & 1:

            @pl.when(xh == 0)
            def _():
                l, acc = all_keys(heads(q_refs[slot], 0, PR), sources, start(0))
                finish(slot, 0, 0, None, l, acc, None)

            @pl.when(xh != 0)
            def _():
                blank(slot, 0)
        else:
            l_s[...], acc_s[...] = start(0)

            def keep(state):
                l_s[...], acc_s[...] = state

            diagonal(
                place,
                d,
                lambda: heads(q_refs[slot], 0, PR),
                sources,
                lambda: (l_s[...], acc_s[...]),
                keep,
            )
            finish(slot, 0, 0, None, l_s[...], acc_s[...], place.query_at(d) >= place.xl * PR)
        for g in range(GR):
            live = place.live(d, g)

            @pl.when(live != 0)
            def _():
                q = heads(q_refs[slot], PR + g * RR, RR)
                state = all_keys(q, sources, start(1 + g))
                if d < 2:
                    l_s[:MR], acc_s[:MR] = state

                    @pl.when(place.other_xh(d) >= xh)
                    def _():
                        l_s[:MR], acc_s[:MR] = plain(q, own_blocks(d, g), (l_s[:MR], acc_s[:MR]))

                    state = l_s[:MR], acc_s[:MR]
                finish(slot, 1 + g, 0, None, *state, None)

            @pl.when(live == 0)
            def _():
                blank(slot, 1 + g)

    @pl.when(jnp.max(bad_s[...]) > 0.0)
    def _():
        copies = [pltpu.make_async_copy(far[i], far_s.at[i], sems.at[i]) for i in range(6)]
        for copy in copies:
            copy.start()
        for copy in copies:
            copy.wait()
        za, zb, pa, pb, ma, mb = (far_s.at[i] for i in range(6))
        row = lax.broadcasted_iota(jnp.int32, (ROWS, 1), 0)
        for slot, d in enumerate(slots):
            xh_d = place.other_xh(d)
            offset = (xh_d - xh) * (16 * 512) + 2 * z * 512 + core * 512 + place.y * 128
            prompt_at = offset + jnp.bitwise_xor(place.xl, d >> 1) * PR + row
            q_at = jnp.where(row < PR, prompt_at, NZ * 2048)
            own_row = (xh_d - xh) * (16 * RR) + (2 * z + core) * RR
            group = jnp.where(row < PR, -1, (row - PR) // RR)
            own_at = own_row + (row - PR) % RR

            @pl.loop(0, HQ)
            def _(h):
                q = q_refs[slot][:, pl.ds(pl.multiple_of(h * DH, DH), DH)]
                m_s[:ROWS] = jnp.full((ROWS, 1), EMPTY, jnp.float32)
                l_s[:ROWS], acc_s[:ROWS] = fresh(ROWS)
                for half, last in ((0, (la, lb)), (1, (ha, hb))):

                    @pl.loop(0, HALF)
                    def _(i):
                        zz = i + half * HALF
                        pieces, values = [], []

                        def add(both, mask):
                            keys, value = split(both)
                            pieces.append(jnp.where(mask, nt(q, keys), MASKED))
                            values.append(value)

                        for (a, b), step, index in (
                            ((za, zb), 0, zz),
                            ((pa, pb), NY - 1, zz),
                            ((ma, mb), 1, zz),
                            (last, 2, i),
                        ):
                            for ref, part in ((a, core), (b, 1 - core)):
                                add(ref[index], place.key_at(step, zz, part, PR) <= q_at)
                        if d < 2:
                            col = lax.broadcasted_iota(jnp.int32, (1, RR), 1)
                            for ref, part in ((oa, core), (ob, 1 - core)):
                                for g in range(GR):
                                    at = (2 * zz + part) * RR + col
                                    add(ref[zz, g], (group == g) & (at <= own_at))
                        m_s[:ROWS], l_s[:ROWS], acc_s[:ROWS] = fold(
                            pieces, values, (m_s[:ROWS], l_s[:ROWS], acc_s[:ROWS])
                        )

                for unit, (first, rows) in enumerate(((0, PR), (PR, RR), (PR + RR, RR))):
                    state = (ref[first : first + rows] for ref in (m_s, l_s, acc_s))
                    finish(slot, unit, h * rows, *state, None)

    eye = lax.broadcasted_iota(jnp.int32, (DH, DH), 0) == lax.broadcasted_iota(
        jnp.int32, (DH, DH), 1
    )
    for slot in range(n):
        lse = [
            jnp.sum(jnp.where(eye, lse_s[slot, b * DH : (b + 1) * DH], 0.0), axis=0, keepdims=True)
            for b in range(LSE_ROWS // DH)
        ]
        lse = jnp.concatenate(lse + [jnp.zeros((1, DH), jnp.float32)], axis=0)
        hi = lse.astype(jnp.bfloat16).astype(jnp.float32)
        mid = (lse - hi).astype(jnp.bfloat16).astype(jnp.float32)
        low = lse - hi - mid
        parts = jnp.concatenate([hi, mid, low, jnp.zeros_like(low)], axis=0)
        outs[slot][HQ * ROWS :] = parts.astype(jnp.bfloat16)


VMEM = pl.BlockSpec(memory_space=pltpu.VMEM)
SMEM = pl.BlockSpec(memory_space=pltpu.SMEM)


def flops(slots, share):
    return pl.CostEstimate(
        flops=int(1_700_000_000 * len(slots) * share), transcendentals=0, bytes_accessed=0
    )


ACC = jax.ShapeDtypeStruct((HQ * ROWS, DH), jnp.float32)
TOTALS = jax.ShapeDtypeStruct((MP, DH), jnp.float32)


def stage(slots, steps, scal, qs, state, *arrays):
    l, *acc = pl.pallas_call(
        functools.partial(stage_kernel, slots, steps, state is not None),
        in_specs=[SMEM] + [VMEM] * (len(slots) + len(arrays) + (1 + len(slots)) * (state is not None)),
        out_specs=[VMEM] * (1 + len(slots)),
        out_shape=[TOTALS] + [ACC] * len(slots),
        compiler_params=pltpu.CompilerParams(vmem_limit_bytes=GRANT),
        cost_estimate=flops(slots, len(steps) / 4),
        name="stage" + "".join(map(str, steps)),
    )(scal, *[qs[d] for d in slots], *([] if state is None else [state[0], *[state[1][d] for d in slots]]), *arrays)
    return l, dict(zip(slots, acc))


def attend(slots, scal, qs, state, near, ready, far):
    n = len(slots)
    return pl.pallas_call(
        functools.partial(attend_kernel, slots, len(near) > 0),
        in_specs=[SMEM]
        + [VMEM] * (2 * n + 1 + len(near) + len(ready))
        + [pl.BlockSpec(memory_space=pl.ANY)] * len(far),
        out_specs=[VMEM] * n,
        out_shape=[jax.ShapeDtypeStruct((PAY, DH), jnp.bfloat16)] * n,
        scratch_shapes=[
            pltpu.VMEM((MP, 1), jnp.float32),
            pltpu.VMEM((MP, 1), jnp.float32),
            pltpu.VMEM((MP, DH), jnp.float32),
            pltpu.VMEM((n, LSE_ROWS, DH), jnp.float32),
            pltpu.VMEM((MP, 1), jnp.float32),
            pltpu.VMEM((6, NZ, PR, 2 * DH), jnp.bfloat16),
            pltpu.SemaphoreType.DMA((6,)),
        ],
        compiler_params=pltpu.CompilerParams(vmem_limit_bytes=GRANT),
        cost_estimate=flops(slots, 3 / 4 if near else 1 / 4),
        name="attend" + "".join(map(str, slots)),
    )(scal, *[qs[d] for d in slots], state[0], *[state[1][d] for d in slots], *near, *ready, *far)


def merge_kernel(live, p0, p1, p2, p3, prompt_out, response_out):
    parts = (p0, p1, p2, p3)
    lses = []
    for p in parts:
        t = p[HQ * ROWS :].astype(jnp.float32)
        lses.append(t[0:8] + t[8:16] + t[16:24])
    top = functools.reduce(jnp.maximum, lses)
    weights = [jnp.exp2(s - top) for s in lses]
    total = functools.reduce(jnp.add, weights)
    weights = [w / total for w in weights]
    stack = jnp.concatenate(weights + [jnp.zeros((DH - 32, DH), jnp.float32)], axis=0)
    cols = jnp.transpose(stack)

    def unit(base, rows, at):
        pieces = []
        for b0 in range(0, rows, DH):
            height = min(DH, rows - b0)
            block = (at + b0) // DH
            acc = None
            for n, p in enumerate(parts):
                w = cols[:height, n * 8 + block : n * 8 + block + 1]
                term = p[base + b0 : base + b0 + height].astype(jnp.float32) * w
                acc = term if acc is None else acc + term
            pieces.append(acc)
        return jnp.concatenate(pieces, axis=0)

    o = unit(0, MP, UNIT_AT[0])
    for h in range(HQ):
        prompt_out[:, h * DH : (h + 1) * DH] = o[h * PR : (h + 1) * PR].astype(jnp.bfloat16)
    row = lax.broadcasted_iota(jnp.int32, (RR, 1), 0)
    for g in range(GR):
        o = unit(MP + g * MR, MR, UNIT_AT[1 + g])
        keep = row < live[g]
        for h in range(HQ):
            response_out[g, :, h * DH : (h + 1) * DH] = jnp.where(
                keep, o[h * RR : (h + 1) * RR], 0.0
            ).astype(jnp.bfloat16)


def merge(live, *parts):
    vmem = pl.BlockSpec(memory_space=pltpu.VMEM)
    return pl.pallas_call(
        merge_kernel,
        in_specs=[pl.BlockSpec(memory_space=pltpu.SMEM)] + [vmem] * 4,
        out_specs=[vmem] * 2,
        out_shape=[
            jax.ShapeDtypeStruct((PR, HQ * DH), jnp.bfloat16),
            jax.ShapeDtypeStruct((GR, RR, HQ * DH), jnp.bfloat16),
        ],
        compiler_params=pltpu.CompilerParams(vmem_limit_bytes=GRANT),
        name="merge",
    )(live, *parts)


def flip_x(value, d):
    return lax.ppermute(value, ("xl", "xh"), [(s, s ^ d) for s in range(NXL * NXH)])


def flip_core(value):
    return lax.ppermute(value, "core", [(0, 1), (1, 0)])


def shift_y(value, step):
    return lax.ppermute(value, "y", [(i, (i + step) % NY) for i in range(NY)])


def copy_for_each(value, axes, count):
    many = jnp.broadcast_to(value[None], (count, *value.shape))
    return lax.all_to_all(many, axes, 0, 0, tiled=True)


def shards(
    prompt_queries,
    prompt_keys,
    prompt_values,
    response_queries,
    response_keys,
    response_values,
    response_lengths,
):
    y, xl, xh, z, core = (lax.axis_index(a).astype(jnp.int32) for a in ("y", "xl", "xh", "z", "core"))

    queries = jnp.concatenate([prompt_queries[0], response_queries.reshape(GR * RR, HQ * DH)], axis=0)
    za = copy_for_each(jnp.concatenate([prompt_keys[0], prompt_values[0]], axis=1), "z", NZ)
    own_kv = jnp.concatenate([response_keys, response_values], axis=2)
    qs = [queries] + [flip_x(queries, d) for d in (1, 2, 3)]
    other_lengths = lax.ppermute(response_lengths, "xl", [(0, 1), (1, 0)])

    block = 2 * z + core
    lengths = jnp.stack([response_lengths, response_lengths, other_lengths, other_lengths])
    blocks = jnp.stack([xh, 1 - xh, xh, 1 - xh]) * 16 + block
    is_live = (blocks[:, None] * RR < lengths).astype(jnp.int32)
    scal = jnp.concatenate([jnp.stack([y, xl, xh, z, core]), is_live.reshape(-1)])

    live_rows = response_lengths - (xh * 16 + block) * RR
    za, scal, live_rows, own_kv, *qs = lax.optimization_barrier((za, scal, live_rows, own_kv, *qs))
    oa = copy_for_each(own_kv, "z", NZ)
    pa, ma = shift_y(za, 1), shift_y(za, -1)
    zb = flip_core(za)
    l, acc = stage((0, 1, 2, 3), (0,), scal, qs, None, za, zb)
    pa, ma, l = lax.optimization_barrier((pa, ma, l))

    la, ha = shift_y(pa[:HALF], 1), shift_y(ma[HALF:], -1)
    pb, mb = flip_core(pa), flip_core(ma)
    l, later = stage((1, 3, 2), (NY - 1, 1), scal, qs, (l, acc), pa, pb, ma, mb)
    la, ha, oa, l = lax.optimization_barrier((la, ha, oa, l))
    lb, hb, ob = flip_core(la), flip_core(ha), flip_core(oa)

    ready, far = (la, lb, ha, hb, oa, ob), (za, zb, pa, pb, ma, mb)
    (pay1,) = attend((1,), scal, qs, (l, later), (), ready, far)
    got1 = flip_x(pay1, 1)
    scal, pay1 = lax.optimization_barrier((scal, pay1))
    pay3, pay2 = attend((3, 2), scal, qs, (l, later), (), ready, far)
    got3, got2 = flip_x(pay3, 3), flip_x(pay2, 2)
    scal, pay3 = lax.optimization_barrier((scal, pay3))
    (pay0,) = attend((0,), scal, qs, (l, acc), (pa, pb, ma, mb), ready, far)
    prompt_out, response_out = merge(live_rows, pay0, got1, got2, got3)
    return prompt_out[None], response_out


def solution(mesh):
    fine = Mesh(mesh.devices.reshape(NY, NXL, NXH, NZ, NC), ("y", "xl", "xh", "z", "core"))
    resp, ctx = ("y", "xl"), ("xh", "z", "core")
    in_specs = (
        P(ctx, resp, None),
        P(ctx, resp, None),
        P(ctx, resp, None),
        P(resp, ctx, None),
        P(resp, ctx, None),
        P(resp, ctx, None),
        P(resp),
    )
    out_specs = (P(ctx, resp, None), P(resp, ctx, None))
    return jax.shard_map(shards, mesh=fine, in_specs=in_specs, out_specs=out_specs, check_vma=False)
```
